32 devices in a mesh: fft: 16 (over z, x, core), scal: 2 (over y).
Axes of the slice: x: 2, y: 2, z: 4, core: 2. Of those that a mesh axis runs over, the one named last changes fastest.
Arguments:
- scalar_state: float32 [2, 2, 256, 256, 128], P('scal', None, 'fft'), may hold values from -12 to 12
- velocity: bfloat16 [3, 256, 256, 256], P(None, 'fft', 'scal'), may hold values from -6 to 6
- species: int32 [2], P('scal'), may hold values from 0 to 63
- kappa_table: float32 [64], replicated, may hold values from 0.1 to 1
- dealias_bound: int32 [2], P('scal'), may hold values from 64 to 85
Outputs:
- new_state: float32 [2, 2, 256, 256, 128], P('scal', None, 'fft')
- kappa: float32 [2], P('scal')
The draws below stay inside these ranges and needn't reach their ends.
All inputs are finite; a program needn't handle non-finite values.
Results may differ from the reference program's by a relative error of at most 0.0027.
Values may be sent and summed in bfloat16 or wider, within the bound.
No kernel may reach another device: no remote copies, remote signals or barrier semaphores. Data moves between devices by JAX's collectives and lax.ppermute only.
A program may use at most 128 MiB of HBM per device.

```python
import math
import jax
import jax.numpy as jnp
from jax import lax

N = 256
SPECIES = 64
SCALARS = 2


def draw_scalar_state(key, part):
    dims_shape = (SCALARS, 2, N, N, N // 2)
    key_base, key_rough, key_scale = jax.random.split(key, 3)
    values = jnp.clip(jax.random.normal(key_base, dims_shape, jnp.float32), -4.0, 4.0)
    roughness = jnp.exp(jax.random.uniform(key_rough, dims_shape, jnp.float32, math.log(0.5), math.log(1.5)))
    ky_float = jnp.arange(N, dtype=jnp.int32).astype(jnp.float32)
    envelope = jnp.sqrt(1.0 + 2.0 * ky_float / (N - 1)).reshape(1, 1, N, 1, 1)
    scalar_scale = jnp.exp(jax.random.uniform(key_scale, (SCALARS, 1, 1, 1, 1), jnp.float32, math.log(0.5), math.log(2.0)))
    return jnp.clip(values * roughness * envelope * scalar_scale, -12.0, 12.0).astype(jnp.float32)


def block_scale(rng, dims, cuts, least, largest):
    loudness, own = 1.0, jax.random.fold_in(rng, 6)
    for position, shards_of in cuts:
        heights = jnp.exp(jax.random.uniform(jax.random.fold_in(own, position), (shards_of,), jnp.float32, least / len(cuts), largest / len(cuts)))
        loudness = loudness * jnp.repeat(heights, dims[position] // shards_of).reshape([-1 if axis == position else 1 for axis in range(len(dims))])
    return loudness


def noise(stream_key, shape, spread, most, cuts=(), kind=jnp.bfloat16):
    entries = jax.random.normal(stream_key, shape, jnp.float32) * spread
    if len(cuts) > 0:
        entries = block_scale(stream_key, shape, cuts, -0.22, 0.18) * entries
    return jnp.clip(entries, min=-most, max=most).astype(kind)


def setup_inputs(seed: int = 0) -> dict:
    keys = jax.random.split(jax.random.key(seed), 6)
    return {
        "scalar_state": draw_scalar_state(jax.random.fold_in(keys[5], 71), 0),
        "velocity": noise(keys[1], (3, N, N, N), 1.0, 6.0, ((1, 16), (2, 2))),
        "species": jax.random.randint(keys[2], (SCALARS,), 0, SPECIES).astype(jnp.int32),
        "kappa_table": jnp.clip(jnp.exp(jax.random.uniform(keys[3], (SPECIES,), jnp.float32, math.log(0.1), math.log(1.0))), 0.1, 1.0),
        "dealias_bound": jax.random.randint(keys[4], (SCALARS,), N // 4, N // 3 + 1).astype(jnp.int32),
    }


cfl_number = 0.2

def twiddle(size_in, size_out, length):
    row_index = jnp.arange(size_in, dtype=jnp.int32)[:, None]
    col_index = jnp.arange(size_out, dtype=jnp.int32)[None, :]
    angles = (row_index * col_index % length).astype(jnp.float32) * (2.0 * math.pi / length)
    norming = 1.0 / math.sqrt(length)
    return (jnp.cos(angles) * norming, jnp.sin(angles) * norming)

def build_tables(length):
    half_len = length // 2
    full_cos, full_sin = twiddle(length, length, length)
    inv_cos, inv_sin = twiddle(half_len, length, length)
    weight = jnp.where(jnp.arange(half_len, dtype=jnp.int32) == 0, 1.0, 2.0).astype(jnp.float32)[:, None]
    fwd_cos, fwd_sin = twiddle(length, half_len, length)
    listed = (full_cos, full_sin, inv_cos * weight, inv_sin * weight, fwd_cos, fwd_sin)
    return tuple((matrix.astype(jnp.bfloat16) for matrix in listed))

def product(formula, operand, matrix):
    return jnp.einsum(formula, operand.astype(jnp.float32), matrix.astype(jnp.float32), precision=lax.Precision.HIGHEST)

def complex_section(real_part, imag_part, cos_matrix, sin_matrix, formula, inverse):
    real_cos = product(formula, real_part, cos_matrix)
    real_sin = product(formula, real_part, sin_matrix)
    imag_cos = product(formula, imag_part, cos_matrix)
    imag_sin = product(formula, imag_part, sin_matrix)
    if inverse:
        return (real_cos - imag_sin, real_sin + imag_cos)
    return (real_cos + imag_sin, imag_cos - real_sin)

def reference(scalar_state, velocity, species, kappa_table, dealias_bound):
    scalar_count = scalar_state.shape[0]
    table_count = kappa_table.shape[0]
    length = scalar_state.shape[2]
    half_len = length // 2
    full_cos, full_sin, inv_cos, inv_sin, fwd_cos, fwd_sin = build_tables(length)
    index_full = jnp.arange(length, dtype=jnp.int32)
    signed = jnp.where(index_full < half_len, index_full, index_full - length).astype(jnp.float32)
    ky_wave = signed[:, None, None]
    kz_wave = signed[None, :, None]
    kx_wave = jnp.arange(half_len, dtype=jnp.int32).astype(jnp.float32)[None, None, :]
    ksquare = kx_wave * kx_wave + ky_wave * ky_wave + kz_wave * kz_wave
    weight = jnp.where(kx_wave == 0.0, 1.0, 2.0).astype(jnp.float32)
    cell_count = float(length) ** 3
    step_size = cfl_number * 2.0 * math.pi / length

    def z_inverse(real_part, imag_part):
        z_section = complex_section(real_part, imag_part, full_cos, full_sin, 'ykx,kz->yzx', True)
        return (z_section[0].astype(jnp.bfloat16), z_section[1].astype(jnp.bfloat16))

    def rest_inverse(real_part, imag_part):
        y_section = complex_section(real_part, imag_part, full_cos, full_sin, 'yzx,yw->zwx', True)
        y_real = y_section[0].astype(jnp.bfloat16)
        y_imag = y_section[1].astype(jnp.bfloat16)
        return product('zwk,kx->zwx', y_real, inv_cos) - product('zwk,kx->zwx', y_imag, inv_sin)

    def gradient_set(real_part, imag_part):
        whole_real, whole_imag = z_inverse(real_part.astype(jnp.bfloat16), imag_part.astype(jnp.bfloat16))
        deriv_real, deriv_imag = z_inverse((-kz_wave * imag_part).astype(jnp.bfloat16), (kz_wave * real_part).astype(jnp.bfloat16))
        results = []
        for wavenumber in (kx_wave, ky_wave):
            grad_real = (-wavenumber * whole_imag.astype(jnp.float32)).astype(jnp.bfloat16)
            grad_imag = (wavenumber * whole_real.astype(jnp.float32)).astype(jnp.bfloat16)
            results.append(rest_inverse(grad_real, grad_imag))
        results.append(rest_inverse(deriv_real, deriv_imag))
        return results

    def advect(gradients):
        total = velocity[0].astype(jnp.float32) * gradients[0]
        total = total + velocity[1].astype(jnp.float32) * gradients[1]
        total = total + velocity[2].astype(jnp.float32) * gradients[2]
        return total.astype(jnp.bfloat16)

    def forward_field(physical):
        real_x = product('zyx,xk->zyk', physical, fwd_cos).astype(jnp.bfloat16)
        imag_x = (-product('zyx,xk->zyk', physical, fwd_sin)).astype(jnp.bfloat16)
        y_section = complex_section(real_x, imag_x, full_cos, full_sin, 'zyk,yw->wzk', False)
        y_real = y_section[0].astype(jnp.bfloat16)
        y_imag = y_section[1].astype(jnp.bfloat16)
        return complex_section(y_real, y_imag, full_cos, full_sin, 'wzk,zv->wvk', False)
    updated_list = []
    kappa_list = []
    for scalar in range(scalar_count):
        start_real = scalar_state[scalar, 0]
        start_imag = scalar_state[scalar, 1]
        energy = start_real * start_real + start_imag * start_imag
        variance = jnp.sum(weight * energy) / cell_count
        mean_grad = jnp.sum(weight * ksquare * energy) / cell_count
        gradients = gradient_set(start_real, start_imag)
        peak_value = jnp.max(jnp.sqrt(gradients[0] * gradients[0] + gradients[1] * gradients[1] + gradients[2] * gradients[2]))
        base_kappa = jnp.sum(jnp.where(species[scalar] == jnp.arange(table_count, dtype=jnp.int32), kappa_table, 0.0))
        kappa_value = base_kappa * peak_value * jnp.sqrt(variance) / (mean_grad + 1e-06)
        factor = jnp.exp(-kappa_value * ksquare * step_size)
        bound = dealias_bound[scalar].astype(jnp.float32)
        dealias_mask = (ksquare <= bound * bound).astype(jnp.float32)
        first_real, first_imag = forward_field(advect(gradients))
        first_real = -dealias_mask * first_real
        first_imag = -dealias_mask * first_imag
        mid_real = factor * (start_real + step_size * first_real)
        mid_imag = factor * (start_imag + step_size * first_imag)
        second_real, second_imag = forward_field(advect(gradient_set(mid_real, mid_imag)))
        second_real = -dealias_mask * second_real
        second_imag = -dealias_mask * second_imag
        new_real = factor * start_real + 0.5 * step_size * (factor * first_real + second_real)
        new_imag = factor * start_imag + 0.5 * step_size * (factor * first_imag + second_imag)
        updated_list.append(jnp.stack([new_real, new_imag]))
        kappa_list.append(kappa_value)
    return (jnp.stack(updated_list), jnp.stack(kappa_list))
```

```python
import functools
import math

import jax
import jax.numpy as jnp
import numpy as np
from jax import lax
from jax.experimental import pallas as pl
from jax.experimental.pallas import tpu as pltpu
from jax.sharding import PartitionSpec as P

cfl_number = 0.2
PAD = 16
F32 = jnp.float32
BF16 = jnp.bfloat16


def twiddle(size_in, size_out, length):
    row_index = np.arange(size_in, dtype=np.int64)[:, None]
    col_index = np.arange(size_out, dtype=np.int64)[None, :]
    angles = (row_index * col_index % length).astype(np.float32) * np.float32(
        2.0 * math.pi / length
    )
    norming = np.float32(1.0 / math.sqrt(length))
    return np.cos(angles) * norming, np.sin(angles) * norming


def tables(length):
    half = length // 2
    bf = lambda a: np.asarray(a, np.float32).astype(jnp.bfloat16)
    cos, sin = (bf(a) for a in twiddle(length, length, length))
    index = np.arange(length)
    wave = np.where(index < half, index, index - length).astype(np.float32)[None, :]
    cos_f, sin_f = cos.astype(np.float32), sin.astype(np.float32)
    inverse = np.concatenate([cos, sin, bf(cos_f * wave), bf(sin_f * wave)])
    weight = np.where(np.arange(half) == 0, 1.0, 2.0).astype(np.float32)[:, None]
    inv_cos, inv_sin = twiddle(half, length, length)
    x_inverse = np.concatenate([bf(inv_cos * weight), bf(-inv_sin * weight)])
    fwd_cos, fwd_sin = twiddle(length, half, length)
    x_forward = np.concatenate([bf(fwd_cos), bf(-fwd_sin)], axis=1)
    return inverse, x_inverse, x_forward


def dot(a, b):
    return jnp.dot(a, b, preferred_element_type=F32)


def split3(value):
    high = value.astype(BF16)
    rest = value - high.astype(F32)
    middle = rest.astype(BF16)
    low = (rest - middle.astype(F32)).astype(BF16)
    return high, middle, low


def stat_rows(values, lanes):
    row = lax.broadcasted_iota(jnp.int32, (PAD, lanes), 0)
    block = jnp.zeros((PAD, lanes), F32)
    for place, value in enumerate(values):
        for part, piece in enumerate(split3(jnp.full((PAD, lanes), value, F32))):
            block = jnp.where(row == 3 * place + part, piece.astype(F32), block)
    return block.astype(BF16)


def stat_read(block, place):
    rows = block.astype(F32)
    at = 3 * place
    return rows[at : at + 1] + rows[at + 1 : at + 2] + rows[at + 2 : at + 3]


def z_inverse_row(table, scratch, pair, row, count, ky_local):
    total = count
    prod = dot(table, pair)
    half = pair.shape[1] // 2
    c, s = prod[:total], prod[total : 2 * total]
    kc, ks = prod[2 * total : 3 * total], prod[3 * total :]
    fields = (
        c[:, :half] - s[:, half:],
        c[:, half:] + s[:, :half],
        -kc[:, half:] - ks[:, :half],
        kc[:, :half] - ks[:, half:],
    )
    for place, field in enumerate(fields):
        scratch[place, pl.ds(row, total, stride=ky_local), :] = field


def flush(scratch, outs, me, tail):
    count, _, lanes = scratch.shape
    size = scratch.shape[1] // len(outs)
    for shift, out in enumerate(outs):
        start = pl.multiple_of((me ^ shift) * size, size)
        for place in range(count):
            out[place * size : (place + 1) * size, :] = scratch[
                place, pl.ds(start, size), :
            ].astype(BF16)
        out[count * size :, :] = tail


def waves(ky_row, length, half):
    shape = (length, half)
    kz = lax.broadcasted_iota(jnp.int32, shape, 0)
    kz = jnp.where(kz < half, kz, kz - length).astype(F32)
    kx = lax.broadcasted_iota(jnp.int32, shape, 1).astype(F32)
    ky = jnp.where(ky_row < half, ky_row, ky_row - length).astype(F32)
    return kx, kx * kx + ky * ky + kz * kz


def first_kernel(n, where, state, table, *rest):
    outs, scratch = rest[:n], rest[n]
    ky_local, length, half = state.shape[1:]
    me = where[0]
    cells = float(length) ** 3

    def step(row, sums):
        real, imag = state[0, row], state[1, row]
        kx, ksquare = waves(me * ky_local + row, length, half)
        energy = real * real + imag * imag
        energy = jnp.where(kx == 0.0, energy, 2.0 * energy)
        pair = jnp.concatenate([real.astype(BF16), imag.astype(BF16)], axis=1)
        z_inverse_row(table[...], scratch, pair, row, length, ky_local)
        fold = lambda v: v.reshape(length // 8, 8, half).sum(axis=0)
        return sums[0] + fold(energy), sums[1] + fold(energy * ksquare)

    zero = jnp.zeros((8, half), F32)
    sums = lax.fori_loop(0, ky_local, step, (zero, zero))
    tail = stat_rows([jnp.sum(v) / cells for v in sums], half)
    flush(scratch, outs, me, tail)


def plane_kernel(n, first, where, velocity, table, x_inverse, x_forward, *rest):
    came = rest[:n]
    outs = rest[n : 2 * n]
    rest = rest[2 * n :]
    if first:
        stats, rest = rest[0], rest[1:]
    pair_w, pair_v, scratch = rest[:3]
    length = table.shape[1]
    half = length // 2
    planes = pl.num_programs(0)
    plane_count = scratch.shape[1] // length
    ky_local = length // n
    me = where[0]
    plane = pl.program_id(0)
    for shift in range(n):
        rows = pl.ds(pl.multiple_of((me ^ shift) * ky_local, ky_local), ky_local)
        for place in range(4):
            target = pair_w if place < 2 else pair_v
            lanes = slice(0, half) if place % 2 == 0 else slice(half, length)
            start = pl.multiple_of((place * plane_count + plane) * ky_local, ky_local)
            target[rows, lanes] = came[shift][pl.ds(start, ky_local), :]
    prod_w = dot(table[...], pair_w[...])
    prod_v = dot(table[: 2 * length], pair_v[...])
    kx = lax.broadcasted_iota(jnp.int32, (1, half), 1).astype(F32)
    c, s = prod_w[:length], prod_w[length : 2 * length]
    kc, ks = prod_w[2 * length : 3 * length], prod_w[3 * length :]
    vc, vs = prod_v[:length], prod_v[length:]
    pack = lambda a, b: jnp.concatenate([a.astype(BF16), b.astype(BF16)], axis=1)
    to_x = pack(
        -kx * (c[:, half:] + s[:, :half]), kx * (c[:, :half] - s[:, half:])
    )
    to_y = pack(-kc[:, half:] - ks[:, :half], kc[:, :half] - ks[:, half:])
    to_z = pack(vc[:, :half] - vs[:, half:], vc[:, half:] + vs[:, :half])
    grad_x, grad_y, grad_z = (dot(d, x_inverse[...]) for d in (to_x, to_y, to_z))
    u = velocity[...]
    total = u[0, 0].astype(F32) * grad_x
    total = total + u[1, 0].astype(F32) * grad_y
    total = total + u[2, 0].astype(F32) * grad_z
    if first:
        size = grad_x * grad_x + grad_y * grad_y + grad_z * grad_z
        size = size.reshape(length // 8, 8, length).max(axis=0)

        @pl.when(plane == 0)
        def _():
            stats[0] = size

        @pl.when(plane > 0)
        def _():
            stats[0] = jnp.maximum(stats[0], size)

    spectral = dot(total.astype(BF16), x_forward[...]).astype(BF16)
    prod = dot(table[: 2 * length], spectral)
    c, s = prod[:length], prod[length:]
    rows = pl.ds(plane, length, stride=plane_count)
    scratch[0, rows, :] = c[:, :half] + s[:, half:]
    scratch[1, rows, :] = c[:, half:] - s[:, :half]

    @pl.when(plane == planes - 1)
    def _():
        tail = jnp.zeros((PAD, half), BF16)
        if first:
            tail = stat_rows([jnp.sqrt(jnp.max(stats[0]))], half)
            size = came[0].shape[0] - PAD
            for place in range(2):
                value = sum(stat_read(came[i][size:, :], place) for i in range(n))
                stats[1 + place, :, :half] = jnp.broadcast_to(value, (8, half))
        flush(scratch, outs, me, tail)


def gather_row(came, pair, me, row, n, ky_local, plane_count):
    half = pair.shape[1] // 2
    for shift in range(n):
        rows = pl.ds(
            pl.multiple_of((me ^ shift) * plane_count, plane_count), plane_count
        )
        for place in range(2):
            start = pl.multiple_of((place * ky_local + row) * plane_count, plane_count)
            pair[rows, place * half : (place + 1) * half] = came[shift][
                pl.ds(start, plane_count), :
            ]


def z_forward(table, pair):
    length = pair.shape[0]
    half = length // 2
    prod = dot(table[: 2 * length], pair[...])
    c, s = prod[:length], prod[length:]
    return c[:, :half] + s[:, half:], c[:, half:] - s[:, :half]


def middle_kernel(n, where, limits, state, stats, table, *rest):
    came, (outs, base, kappa_out) = rest[:n], (rest[n : 2 * n], *rest[2 * n : 2 * n + 2])
    pair, scratch = rest[2 * n + 2 :]
    ky_local, length, half = state.shape[1:]
    plane_count = length // n
    me = where[0]
    dt = cfl_number * 2.0 * math.pi / length
    size = came[0].shape[0] - PAD
    peak = stat_read(came[0][size:, :], 0)
    for shift in range(1, n):
        peak = jnp.maximum(peak, stat_read(came[shift][size:, :], 0))
    variance, gradsq = stats[1, :1, :half], stats[2, :1, :half]
    kappa = limits[0] * peak * jnp.sqrt(variance) / (gradsq + 1e-06)
    kappa_out[...] = jnp.broadcast_to(kappa, (8, half))

    def step(row, carry):
        gather_row(came, pair, me, row, n, ky_local, plane_count)
        real, imag = z_forward(table, pair)
        _, ksquare = waves(me * ky_local + row, length, half)
        factor = jnp.exp(-kappa * ksquare * dt)
        gain = jnp.where(ksquare <= limits[1], -dt, 0.0)
        both = []
        for place, part in enumerate((real, imag)):
            start = factor * state[place, row]
            middle = start + factor * (gain * part)
            base[place, row] = 0.5 * (start + middle)
            both.append(middle.astype(BF16))
        z_inverse_row(
            table[...], scratch, jnp.concatenate(both, axis=1), row, length, ky_local
        )
        return carry

    lax.fori_loop(0, ky_local, step, 0)
    flush(scratch, outs, me, jnp.zeros((PAD, half), BF16))


def last_kernel(n, where, limits, base, table, *rest):
    came, out, pair = rest[:n], rest[n], rest[n + 1]
    ky_local, length, half = base.shape[1:]
    me = where[0]
    dt = cfl_number * 2.0 * math.pi / length

    def step(row, carry):
        gather_row(came, pair, me, row, n, ky_local, length // n)
        real, imag = z_forward(table, pair)
        _, ksquare = waves(me * ky_local + row, length, half)
        gain = jnp.where(ksquare <= limits[1], -0.5 * dt, 0.0)
        out[0, row] = base[0, row] + gain * real
        out[1, row] = base[1, row] + gain * imag
        return carry

    lax.fori_loop(0, ky_local, step, 0)


VM = pl.BlockSpec(memory_space=pltpu.VMEM)
SM = pl.BlockSpec(memory_space=pltpu.SMEM)


def exchange(parts, axis, n):
    moved = [parts[0]]
    for shift in range(1, n):
        pairs = [(i, i ^ shift) for i in range(n)]
        moved.append(lax.ppermute(parts[shift], axis, pairs))
    return moved


def gather_velocity(velocity, groups):
    mine = lax.axis_index("scal")
    rows = velocity.shape[2]
    shape = (*velocity.shape[:2], rows * groups, velocity.shape[3])
    whole = jnp.zeros(shape, velocity.dtype)
    for shift in range(groups):
        piece = velocity
        if shift:
            pairs = [((i + shift) % groups, i) for i in range(groups)]
            piece = lax.ppermute(velocity, "scal", pairs)
        start = (mine + shift) % groups * rows
        whole = lax.dynamic_update_slice_in_dim(whole, piece, start, axis=2)
    return whole


def body(n, groups, scalar_state, velocity, species, kappa_table, dealias_bound):
    state = scalar_state[0]
    ky_local, length, half = state.shape[1:]
    planes = length // n
    table, x_inverse, x_forward = (jnp.asarray(t) for t in tables(length))
    where = lax.axis_index("fft").astype(jnp.int32).reshape(1)
    matches = species[0] == jnp.arange(kappa_table.shape[0], dtype=jnp.int32)
    base_kappa = jnp.sum(jnp.where(matches, kappa_table, 0.0))
    bound = dealias_bound[0].astype(F32)
    limits = jnp.stack([base_kappa, bound * bound])
    message = lambda fields: jax.ShapeDtypeStruct(
        (fields * planes * ky_local + PAD, half), BF16
    )
    params = pltpu.CompilerParams(vmem_limit_bytes=58 << 20)
    z_scratch = pltpu.VMEM((4, length * ky_local, half), F32)
    pair_scratch = pltpu.VMEM((length, length), BF16)

    sent = pl.pallas_call(
        functools.partial(first_kernel, n),
        out_shape=[message(4)] * n,
        in_specs=[SM, VM, VM],
        out_specs=[VM] * n,
        scratch_shapes=[z_scratch],
        compiler_params=params,
        name="first",
    )(where, state, table)
    came = exchange(sent, "fft", n)
    speeds = gather_velocity(velocity, groups)

    def planes_call(first, came):
        whole = lambda shape: pl.BlockSpec(
            shape, lambda i: (0,) * len(shape), pipeline_mode=pl.Buffered(1)
        )
        shapes = [message(2)] * n
        specs = [pl.BlockSpec(memory_space=pltpu.VMEM)] * n
        if first:
            shapes = shapes + [jax.ShapeDtypeStruct((3, 8, length), F32)]
            specs = specs + [pl.BlockSpec(memory_space=pltpu.VMEM)]
        return pl.pallas_call(
            functools.partial(plane_kernel, n, first),
            out_shape=shapes,
            grid=(planes,),
            in_specs=[
                SM,
                pl.BlockSpec((3, 1, length, length), lambda i: (0, i, 0, 0)),
                *[VM] * 3,
                *[VM] * n,
            ],
            out_specs=specs,
            scratch_shapes=[
                pair_scratch,
                pair_scratch,
                pltpu.VMEM((2, length * planes, half), F32),
            ],
            compiler_params=params,
            name="planes",
        )(where, speeds, table, x_inverse, x_forward, *came)

    *sent, stats = planes_call(True, came)
    came = exchange(sent, "fft", n)
    *sent, base, kappa = pl.pallas_call(
        functools.partial(middle_kernel, n),
        out_shape=[message(4)] * n
        + [
            jax.ShapeDtypeStruct(state.shape, F32),
            jax.ShapeDtypeStruct((8, half), F32),
        ],
        in_specs=[SM, SM] + [VM] * (3 + n),
        out_specs=[VM] * (n + 2),
        scratch_shapes=[pair_scratch, z_scratch],
        compiler_params=params,
        name="middle",
    )(where, limits, state, stats, table, *came)
    came = exchange(sent, "fft", n)
    sent = planes_call(False, came)
    came = exchange(sent, "fft", n)
    new_state = pl.pallas_call(
        functools.partial(last_kernel, n),
        out_shape=jax.ShapeDtypeStruct(state.shape, F32),
        in_specs=[SM, SM] + [VM] * (2 + n),
        out_specs=VM,
        scratch_shapes=[pair_scratch],
        compiler_params=params,
        name="last",
    )(where, limits, base, table, *came)
    return new_state[None], kappa[0, :1]


def solution(mesh):
    placed = (
        P("scal", None, "fft", None, None),
        P(None, "fft", "scal", None),
        P("scal"),
        P(),
        P("scal"),
    )
    return jax.shard_map(
        functools.partial(body, mesh.shape["fft"], mesh.shape["scal"]),
        mesh=mesh,
        in_specs=placed,
        out_specs=(P("scal", None, "fft", None, None), P("scal")),
        check_vma=False,
    )
```
